256 devices in a mesh: grp: 4 (over z_hi), freq: 64 (over z_lo, y, x, core).
Axes of the slice: x: 4, y: 4, z: 8 (z_hi: 4, z_lo: 2; z = z_hi * 2 + z_lo), core: 2. Of those that a mesh axis runs over, the one named last changes fastest.
Arguments:
- sources: bfloat16 [1024, 262144], P('freq', 'grp'), may hold values from -6 to 6
- panel_pos: float32 [3, 262144], P(None, 'grp'), may hold values from -1 to 1
- panel_blade: int32 [262144], P('grp'), may hold values from 0 to 3
- observer_table: float32 [3, 2048], replicated, may hold values from -8 to 8, as said below
- observer_index: int32 [32], replicated, may hold values from 0 to 2047
Outputs:
- spectra: float32 [512, 4, 2, 32], P('freq', 'grp')
The draws below stay inside these ranges and needn't reach their ends.
Inputs may be any that keep to these rules, and one draw needn't show every extreme that they name: `observer_table`: each observer lies 3 to 8 units from the anchor (0, 0, 0).
All inputs are finite; a program needn't handle non-finite values.
Results may differ from the reference program's by a relative error of at most 0.0047.
Values may be sent and summed in bfloat16 or wider, within the bound.
No kernel may reach another device: no remote copies, remote signals or barrier semaphores. Data moves between devices by JAX's collectives and lax.ppermute only.
A program may use at most 64 MiB of HBM per device.

```python
import math
import jax
import jax.numpy as jnp
from jax import lax

NT = 1024
NF = 512
NCOMP = 4
NOBS = 32
NOBS_ALL = 2048
PANELS = 262144


def draw_observer_table(key, part):
    key_height = jax.random.fold_in(key, 11)
    key_turn = jax.random.fold_in(key, 12)
    key_radius = jax.random.fold_in(key, 13)
    height = jax.random.uniform(key_height, (NOBS_ALL,), jnp.float32, -1.0, 1.0)
    turn_angle = jax.random.uniform(key_turn, (NOBS_ALL,), jnp.float32, -math.pi, math.pi)
    uniform_part = jax.random.uniform(key_radius, (NOBS_ALL,), jnp.float32, 0.0, 1.0)
    radius = 3.0 + 5.0 * uniform_part
    cycle_radius = jnp.sqrt(jnp.maximum(1.0 - height * height, 0.0))
    return jnp.stack([radius * cycle_radius * jnp.cos(turn_angle), radius * cycle_radius * jnp.sin(turn_angle), radius * height]).astype(jnp.float32)


def place_ends(result, own_key, least, largest):
    spot = [jax.random.randint(jax.random.fold_in(own_key, axis), (), 0, length) for axis, length in enumerate(result.shape)]
    widest = result.shape.index(max(result.shape))
    beside = spot[:widest] + [(spot[widest] + 1) % result.shape[widest]] + spot[widest + 1:]
    return result.at[tuple(spot)].set(least).at[tuple(beside)].set(largest)


def level_of(rng, dims, shards, low, largest):
    gain = 1.0
    for position, blocks in shards:
        draws = jax.random.uniform(jax.random.fold_in(jax.random.fold_in(rng, 6), position), (blocks,), jnp.float32, low / len(shards), largest / len(shards))
        gain = gain * jnp.repeat(jnp.exp(draws), dims[position] // blocks).reshape((-1,) + (1,) * (len(dims) - 1 - position))
    return gain


def normal_values(own_key, shape, deviation, limit, split=(), kind=jnp.bfloat16):
    drawn = deviation * jax.random.normal(own_key, shape, jnp.float32)
    if split:
        drawn = drawn * level_of(own_key, shape, split, -0.22, 0.18)
    return jnp.clip(drawn, -limit, limit).astype(kind)


def setup_inputs(seed: int = 0) -> dict:
    arg_keys = jax.random.split(jax.random.key(seed), 6)
    return {
        "sources": normal_values(arg_keys[0], (NT, PANELS), 1.0, 6.0, ((0, 64), (1, 4))),
        "panel_pos": jnp.clip(jax.random.uniform(arg_keys[1], (3, PANELS), jnp.float32, -1.0, 1.0) * level_of(arg_keys[1], (3, PANELS), ((1, 4),), -0.4, 0.0), -1.0, 1.0),
        "panel_blade": place_ends(jax.random.randint(arg_keys[2], (PANELS,), 0, NCOMP), jax.random.fold_in(arg_keys[2], 1), 0, NCOMP - 1).astype(jnp.int32),
        "observer_table": draw_observer_table(jax.random.fold_in(arg_keys[5], 71), 0),
        "observer_index": place_ends(jax.random.randint(arg_keys[4], (NOBS,), 0, NOBS_ALL), jax.random.fold_in(arg_keys[4], 1), 0, NOBS_ALL - 1).astype(jnp.int32),
    }


wave_step = 0.04

def transform_table():
    row_index = jnp.arange(2 * NF, dtype=jnp.int32)
    samples = jnp.arange(NT, dtype=jnp.int32)
    frequency = row_index // 2
    parity = row_index % 2
    turn_count = frequency[:, None] * samples[None, :] % NT
    angle_table = 2.0 * math.pi / NT * turn_count.astype(jnp.float32)
    values = jnp.where(parity[:, None] == 0, jnp.cos(angle_table), -jnp.sin(angle_table))
    return (values / math.sqrt(NT)).astype(jnp.bfloat16)

def distances(positions, observers):
    offset_x = observers[0][:, None] - positions[0][None, :]
    offset_y = observers[1][:, None] - positions[1][None, :]
    offset_z = observers[2][:, None] - positions[2][None, :]
    return jnp.sqrt(offset_x * offset_x + offset_y * offset_y + offset_z * offset_z)

def blade_masks(blades):
    return (blades[None, :] == jnp.arange(NCOMP, dtype=jnp.int32)[:, None]).astype(jnp.bfloat16)

def frequency_term(frequency, spectrum_pair, blade_mask, distance, amplitude):
    wavenumber = wave_step * frequency.astype(jnp.float32)
    phase_angle = wavenumber * distance
    green_matrix = jnp.concatenate([jnp.cos(phase_angle) * amplitude, -jnp.sin(phase_angle) * amplitude], axis=0).astype(jnp.bfloat16)
    weighted = jnp.concatenate([spectrum_pair[0][None, :] * blade_mask, spectrum_pair[1][None, :] * blade_mask], axis=0)
    product = lax.dot_general(weighted, green_matrix, (((1,), (1,)), ((), ())), preferred_element_type=jnp.float32)
    blade_count = blade_mask.shape[0]
    observer_count = distance.shape[0]
    real_part = product[:blade_count, :observer_count] - product[blade_count:, observer_count:]
    imag_part = product[:blade_count, observer_count:] + product[blade_count:, :observer_count]
    return jnp.stack([real_part, imag_part], axis=1)

def reference(sources, panel_pos, panel_blade, observer_table, observer_index):
    observers = observer_table[:, observer_index]
    spectrum = jnp.dot(transform_table(), sources, preferred_element_type=jnp.float32).astype(jnp.bfloat16)
    spectrum = spectrum.reshape(NF, 2, spectrum.shape[1])
    distance = distances(panel_pos, observers)
    amplitude = 0.25 / (math.pi * distance)
    blade_mask = blade_masks(panel_blade)

    def per_frequency(element):
        return frequency_term(element[0], element[1], blade_mask, distance, amplitude)
    return lax.map(per_frequency, (jnp.arange(NF, dtype=jnp.int32), spectrum))
```

```python
import functools
import math

import jax
import jax.numpy as jnp
from jax import lax
from jax.experimental import pallas as pl
from jax.experimental.pallas import tpu as pltpu
from jax.sharding import PartitionSpec as P

NT = 1024
NF = 512
NCOMP = 4
QUAD = 4
BLOCK = 4
F32, BF16 = jnp.float32, jnp.bfloat16

wave_step = 0.04


def transform_table():
    samples = jnp.arange(NT, dtype=jnp.int32)
    small = jnp.arange(32, dtype=jnp.int32)
    turn = 2.0 * math.pi / NT
    low = turn * (small[:, None] * samples[None, :] % NT).astype(F32)
    high = turn * (32 * small[: NF // 32, None] * samples[None, :] % NT).astype(F32)
    cl, sl = jnp.cos(low), jnp.sin(low)
    scale = 1.0 / math.sqrt(NT)
    ch, sh = jnp.cos(high) * scale, jnp.sin(high) * scale
    cl, sl, ch, sh = lax.optimization_barrier((cl, sl, ch, sh))
    re = ch[:, None] * cl[None] - sh[:, None] * sl[None]
    im = -(sh[:, None] * cl[None] + ch[:, None] * sl[None])
    return jnp.stack([re, im], axis=2).reshape(2 * NF, NT).astype(BF16)


def green_start(positions, observers):
    columns = positions.T
    lane_observers = jnp.tile(observers, (1, QUAD))
    offset_x = lane_observers[0][None, :] - columns[:, 0:1]
    offset_y = lane_observers[1][None, :] - columns[:, 1:2]
    offset_z = lane_observers[2][None, :] - columns[:, 2:3]
    distance = jnp.sqrt(offset_x * offset_x + offset_y * offset_y + offset_z * offset_z)
    amplitude = 0.25 / (math.pi * distance)
    offset = jnp.repeat(jnp.arange(QUAD, dtype=F32), observers.shape[1])
    near = (wave_step * (offset - QUAD))[None, :] * distance
    far = (wave_step * (offset - 2 * QUAD))[None, :] * distance
    turn = 2.0 * jnp.cos((wave_step * QUAD) * distance)
    return (
        turn,
        jnp.cos(near) * amplitude,
        -jnp.sin(near) * amplitude,
        jnp.cos(far) * amplitude,
        -jnp.sin(far) * amplitude,
    )


def radiate_kernel(
    table_ref, source_ref, turn_ref, c1_ref, s1_ref, c2_ref, s2_ref, blade_ref, out_ref,
    spectrum, masks, ca, sa, cb, sb, green_a, green_b,
):
    panels = source_ref.shape[1]
    quads = NF // QUAD
    spectrum[...] = jnp.dot(table_ref[...], source_ref[...], preferred_element_type=F32).astype(BF16)
    for b in range(NCOMP):
        masks[b] = jnp.broadcast_to(
            jnp.where(blade_ref[...] == b, 1.0, 0.0), (16, panels)
        ).astype(BF16)
    ca[...] = c1_ref[...]
    sa[...] = s1_ref[...]
    cb[...] = c2_ref[...]
    sb[...] = s2_ref[...]
    row = lax.broadcasted_iota(jnp.int32, (8, 128), 0)
    lane = lax.broadcasted_iota(jnp.int32, (8, 128), 1)
    diagonal = (row // 2) == (lane // 32)
    even = (row % 2) == 0

    def generate(green):
        for chunk in range(panels // 16):
            rows = pl.ds(16 * chunk, 16)
            turn = turn_ref[rows, :]
            c, s, cp, sp = ca[rows, :], sa[rows, :], cb[rows, :], sb[rows, :]
            for k in range(BLOCK):
                c, cp = turn * c - cp, c
                s, sp = turn * s - sp, s
                green[k, rows, 0:128] = c.astype(BF16)
                green[k, rows, 128:256] = s.astype(BF16)
            ca[rows, :] = c
            sa[rows, :] = s
            cb[rows, :] = cp
            sb[rows, :] = sp

    def contract(block, green):
        for pair in range(BLOCK // 2):
            start = block * (BLOCK * 8) + pair * 16
            part = spectrum[pl.ds(pl.multiple_of(start, 16), 16), :]
            weighted = jnp.concatenate([part * masks[b] for b in range(NCOMP)], axis=0)
            for k2 in range(2):
                k = pair * 2 + k2
                r = jnp.dot(weighted, green[k], preferred_element_type=F32)
                acc_re = None
                for b in range(NCOMP):
                    top = 16 * b + 8 * k2
                    u = r[top : top + 8, 0:128]
                    v = r[top : top + 8, 128:256]
                    w = jnp.where(even, -pltpu.roll(v, 7, 0), pltpu.roll(v, 1, 0))
                    z = jnp.where(diagonal, u + w, 0.0)
                    if b:
                        z = pltpu.roll(z, 2 * b, 0)
                    acc_re = z if acc_re is None else acc_re + z
                y = acc_re
                for j in range(1, QUAD):
                    y = jnp.where(lane // 32 == j, pltpu.roll(acc_re, 8 - 2 * j, 0), y)
                out_ref[block * BLOCK + k] = y

    generate(green_a)

    def step(i, carry):
        generate(green_b)
        contract(2 * i, green_a)
        generate(green_a)
        contract(2 * i + 1, green_b)
        return carry

    lax.fori_loop(0, quads // BLOCK // 2, step, 0)


def radiate(table, exchanged, start, blades, interpret=False):
    panels = exchanged.shape[1]
    quads = NF // QUAD
    vm = pl.BlockSpec(memory_space=pltpu.VMEM)
    state = pltpu.VMEM((panels, 128), F32)
    return pl.pallas_call(
        radiate_kernel,
        out_shape=jax.ShapeDtypeStruct((quads, 8, 128), F32),
        in_specs=[vm] * 8,
        out_specs=vm,
        scratch_shapes=[
            pltpu.VMEM((2 * NF, panels), BF16),
            pltpu.VMEM((NCOMP, 16, panels), BF16),
            state, state, state, state,
            pltpu.VMEM((BLOCK, panels, 256), BF16),
            pltpu.VMEM((BLOCK, panels, 256), BF16),
        ],
        compiler_params=pltpu.CompilerParams(vmem_limit_bytes=48 * 1024 * 1024),
        cost_estimate=pl.CostEstimate(flops=20_000_000_000, bytes_accessed=8_000_000, transcendentals=0),
        name="radiate",
    )(table, exchanged, *start, blades[None, :])


def body(sources, panel_pos, panel_blade, observer_table, observer_index):
    width = sources.shape[1] // lax.axis_size("freq")
    position = lax.axis_index("freq")
    observers = observer_table[:, observer_index]
    exchanged = lax.all_to_all(sources, "freq", split_axis=1, concat_axis=0, tiled=True)
    table = transform_table()
    own_pos = lax.dynamic_slice_in_dim(panel_pos, position * width, width, 1)
    own_blade = lax.dynamic_slice_in_dim(panel_blade, position * width, width, 0)
    start = green_start(own_pos, observers)
    partial = radiate(table, exchanged, start, own_blade)
    owners = lax.axis_size("freq")
    blocks = partial.reshape(owners, NF // QUAD // owners, NCOMP, 2, 128)
    blocks = blocks.transpose(0, 2, 1, 3, 4).astype(BF16)
    blocks = blocks.reshape(owners * NCOMP, -1, 128)
    arrived = lax.all_to_all(blocks, ("freq", "grp"), split_axis=0, concat_axis=0, tiled=True)
    total = arrived.astype(F32).sum(0)
    total = total.reshape(-1, 2, QUAD, observers.shape[1]).transpose(0, 2, 1, 3)
    return total.reshape(NF // owners, 1, 2, observers.shape[1])


def solution(mesh):
    in_specs = (P("freq", "grp"), P(None, "grp"), P("grp"), P(), P())
    out_specs = P("freq", "grp", None, None)
    return jax.shard_map(body, mesh=mesh, in_specs=in_specs, out_specs=out_specs, check_vma=False)
```

```python
import functools
import math

import jax
import jax.numpy as jnp
from jax import lax
from jax.experimental import pallas as pl
from jax.experimental.pallas import tpu as pltpu
from jax.sharding import PartitionSpec as P

NT = 1024
NF = 512
NCOMP = 4
QUAD = 4
BLOCK = 16
STREAMS = 2
GROUP = 2
POP = 1
F32, BF16 = jnp.float32, jnp.bfloat16

wave_step = 0.04


def transform_table():
    samples = jnp.arange(NT, dtype=jnp.int32)
    low_row = jnp.arange(64, dtype=jnp.int32)
    high_row = jnp.arange(NF // 32, dtype=jnp.int32)
    turn = 2.0 * math.pi / NT
    low_count = ((low_row // 2)[:, None] * samples[None, :] + (NT // 4) * (low_row % 2)[:, None]) % NT
    high_count = 32 * high_row[:, None] * samples[None, :] % NT
    low = turn * low_count.astype(F32)
    high = turn * high_count.astype(F32)
    scale = 1.0 / math.sqrt(NT)
    cl, sl = jnp.cos(low), jnp.sin(low)
    ch, sh = jnp.cos(high) * scale, jnp.sin(high) * scale
    cl, sl, ch, sh = lax.optimization_barrier((cl, sl, ch, sh))
    rows = ch[:, None] * cl[None] - sh[:, None] * sl[None]
    return rows.astype(BF16).reshape(2 * NF, NT)


def prepare_kernel(column_ref, observer_ref, out_ref):
    offset = (lax.broadcasted_iota(jnp.int32, (16, 128), 1) // 32 - QUAD).astype(F32) * wave_step
    observers = [jnp.broadcast_to(observer_ref[i : i + 1, :], (16, 128)) for i in range(3)]

    def cos_sin(x):
        x2 = x * x
        c, s = 1.0 / math.factorial(14), 1.0 / math.factorial(15)
        c, s = -c, -s
        for n in range(6, -1, -1):
            sign = 1.0 if n % 2 == 0 else -1.0
            c = c * x2 + sign / math.factorial(2 * n)
            s = s * x2 + sign / math.factorial(2 * n + 1)
        return c, s * x

    def step(i, carry):
        rows = pl.ds(pl.multiple_of(16 * i, 16), 16)
        square = None
        for axis in range(3):
            diff = observers[axis] - column_ref[rows, axis : axis + 1]
            square = diff * diff if square is None else square + diff * diff
        distance = jnp.sqrt(square)
        amplitude = 0.25 / (math.pi * distance)
        cn, sn = cos_sin(offset * distance)
        cq, sq = cos_sin((wave_step * QUAD) * distance)
        c1, s1 = cn * amplitude, -sn * amplitude
        out_ref[0, rows, :] = 2.0 * cq
        out_ref[1, rows, :] = c1
        out_ref[2, rows, :] = s1
        out_ref[3, rows, :] = c1 * cq - s1 * sq
        out_ref[4, rows, :] = s1 * cq + c1 * sq
        return carry

    lax.fori_loop(0, out_ref.shape[1] // 16, step, 0)


def green_start(positions, observers):
    panels = positions.shape[1]
    vm = pl.BlockSpec(memory_space=pltpu.VMEM)
    return pl.pallas_call(
        prepare_kernel,
        out_shape=jax.ShapeDtypeStruct((5, panels, 128), F32),
        in_specs=[vm, vm],
        out_specs=vm,
        compiler_params=pltpu.CompilerParams(vmem_limit_bytes=8 * 1024 * 1024),
        cost_estimate=pl.CostEstimate(flops=20_000_000, bytes_accessed=3_000_000, transcendentals=0),
        name="prepare",
    )(positions.T, jnp.tile(observers, (1, QUAD)))


def radiate_kernel(
    zero_ref, table_hbm, source_hbm, start_ref, blade_ref, out_ref,
    table_ref, source_ref, spectrum, masks, weighted, green_a, green_b, sems, *states
):
    panels = source_ref.shape[1]
    share = panels // STREAMS
    blocks = NF // QUAD // BLOCK
    tiles = panels // 256
    pairs = BLOCK // 2
    chunks = panels // 16
    row = lax.broadcasted_iota(jnp.int32, (8, 128), 0)
    lane = lax.broadcasted_iota(jnp.int32, (8, 128), 1)
    diagonal = (row // 2) == (lane // 32)
    even = (row % 2) == 0
    zero = zero_ref[0]

    table_copies = [
        pltpu.make_async_copy(table_hbm.at[pl.ds(h * NF, NF), :], table_ref.at[pl.ds(h * NF, NF), :], sems.at[h])
        for h in range(2)
    ]
    copies = [
        pltpu.make_async_copy(start_ref.at[:, pl.ds(s * share, share), :], states[s], sems.at[2 + s])
        for s in range(STREAMS)
    ]
    source_copies = [
        pltpu.make_async_copy(
            source_hbm.at[pl.ds(256 * k, 256), :], source_ref.at[pl.ds(256 * k, 256), :], sems.at[2 + STREAMS + k]
        )
        for k in range(4)
    ]
    for c in [table_copies[0], *source_copies, *copies, table_copies[1]]:
        c.start()

    def generate(green, stream, slot):
        own = pl.multiple_of(slot * 16, 16)
        rows = pl.ds(own, 16)
        put = pl.ds(pl.multiple_of(own + stream * share, 16), 16)
        state = states[stream]
        turn, c, s, cp, sp = [state[i, rows, :] for i in range(5)]
        for k in range(BLOCK):
            c, cp = turn * c - cp, c
            s, sp = turn * s - sp, s
            green[k, put, 0:128] = c.astype(BF16)
            green[k, put, 128:256] = s.astype(BF16)
        for i, value in enumerate((c, s, cp, sp)):
            state[i + 1, rows, :] = value

    half_row = lax.broadcasted_iota(jnp.int32, (16, panels), 0) // 8
    for p in range(NCOMP // 2):
        masks[p] = jnp.where(blade_ref[...] == half_row + 2 * p, 1.0, 0.0).astype(BF16)

    def transform(*acc):
        half = NF
        steps = 2 * (tiles // 2) * 4
        per = chunks // STREAMS

        def drain(n, h):
            for m in range(2):
                rows = pltpu.matmul_pop(acc[2 * h + m]).reshape(half // 8, 8, 256)
                spectrum[pl.ds(h * half // 8, half // 8), :, pl.ds((2 * n + m) * 256, 256)] = (
                    jnp.concatenate([rows, rows], axis=1).astype(BF16)
                )

        pending = None
        done = 0
        step = 0
        for n in range(tiles // 2):
            for h in range(2):
                if n == 0:
                    table_copies[h].wait()
                for k in range(4):
                    if n == 0 and h == 0:
                        source_copies[k].wait()
                    for m in range(2):
                        pltpu.matmul_push_rhs(
                            source_ref[pl.ds(256 * k, 256), pl.ds((2 * n + m) * 256, 256)],
                            staging_register=k % 2, mxu_index=m,
                        )
                    for m in range(2):
                        pltpu.matmul_acc_lhs(
                            acc[2 * h + m], table_ref[pl.ds(h * half, half), pl.ds(256 * k, 256)],
                            load_staged_rhs=k % 2,
                        )
                    step += 1
                    if step == 2:
                        for c in copies:
                            c.wait()
                    if step > 2:
                        want = (step - 2) * per // (steps - 2)
                        for slot in range(done, want):
                            for stream in range(STREAMS):
                                generate(green_a, stream, lax.rem(zero + slot, per))
                        done = want
                    if k == 0 and pending is not None:
                        drain(*pending)
                pending = (n, h)
        drain(*pending)

    pl.run_scoped(
        transform,
        pltpu.ACC(0)((NF, 256), F32), pltpu.ACC(1)((NF, 256), F32),
        pltpu.ACC(0)((NF, 256), F32), pltpu.ACC(1)((NF, 256), F32),
    )

    def weigh(q, slot):
        for m in range(2):
            part = spectrum[jnp.minimum(q + m, NF // QUAD - 1)]
            for p in range(NCOMP // 2):
                weighted[2 * slot + m, pl.ds(16 * p, 16), :] = part * masks[p]

    def finish(half_q, m, r):
        total = None
        for b in range(NCOMP):
            top = 8 * b
            u = r[top : top + 8, 0:128]
            v = r[top : top + 8, 128:256]
            w = jnp.where(even, -pltpu.roll(v, 7, 0), pltpu.roll(v, 1, 0))
            z = jnp.where(diagonal, u + w, 0.0)
            if b:
                z = pltpu.roll(z, 2 * b, 0)
            total = z if total is None else total + z
        y = total
        for j in range(1, QUAD):
            y = jnp.where(lane // 32 == j, pltpu.roll(total, 8 - 2 * j, 0), y)
        for b in range(NCOMP):
            out_ref[half_q, b, pl.ds(2 * m, 2), :] = y[2 * b : 2 * b + 2]

    def contract(*acc):
        trips = pairs // GROUP
        local = chunks // trips // STREAMS

        def trip(block, ii, now, later):
            made = 0
            units = [(pair, t) for pair in range(GROUP) for t in range(tiles)]

            def push(pair, t):
                for m in range(2):
                    pltpu.matmul_push_rhs(
                        now[2 * (GROUP * ii + pair) + m, pl.ds(256 * t, 256), :],
                        staging_register=t % 2, mxu_index=m,
                    )

            def accumulate(pair, t):
                for m in range(2):
                    pltpu.matmul_acc_lhs(
                        acc[2 * (pair % 2) + m], weighted[2 * (pair % 2) + m, :, pl.ds(256 * t, 256)],
                        load_staged_rhs=t % 2,
                    )

            def drain(half_q, pair):
                for m in range(2):
                    finish(half_q, m, pltpu.matmul_pop(acc[2 * (pair % 2) + m]))

            def produce(u):
                for n in range(u * local // len(units), (u + 1) * local // len(units)):
                    for stream in range(STREAMS):
                        generate(later, stream, ii * local + lax.rem(zero + n, local))

            for u, (pair, t) in enumerate(units):
                h0 = block * pairs + GROUP * ii + pair
                push(pair, t)
                accumulate(pair, t)
                produce(u)
                if t == POP:
                    weigh(2 * h0 + 2, 1 - pair % 2)
                    if pair:
                        drain(h0 - 1, pair - 1)
            drain(h0, GROUP - 1)

        def step(i, carry):
            def first(ii, c):
                trip(2 * i, ii, green_a, green_b)
                return c

            def second(ii, c):
                trip(2 * i + 1, ii, green_b, green_a)
                return c

            lax.fori_loop(0, trips, first, 0)
            lax.fori_loop(0, trips, second, 0)
            return carry

        for a in acc:
            pltpu.matmul_pop(a)
        weigh(0, 0)
        lax.fori_loop(0, blocks // 2, step, 0)
    pl.run_scoped(contract, *[pltpu.ACC(n % 2)((32, 256), F32) for n in range(4)])


def radiate(table, exchanged, start, blades):
    panels = exchanged.shape[1]
    quads = NF // QUAD
    vm = pl.BlockSpec(memory_space=pltpu.VMEM)
    hbm = pl.BlockSpec(memory_space=pltpu.HBM)
    zero = jnp.minimum(blades[:1], 0)
    return pl.pallas_call(
        radiate_kernel,
        out_shape=jax.ShapeDtypeStruct((quads // 2, NCOMP, 4, 128), F32),
        in_specs=[pl.BlockSpec(memory_space=pltpu.SMEM), hbm, hbm, hbm, vm],
        out_specs=vm,
        scratch_shapes=[
            pltpu.VMEM((2 * NF, NT), BF16),
            pltpu.VMEM((NT, panels), BF16),
            pltpu.VMEM((NF // QUAD, 16, panels), BF16),
            pltpu.VMEM((NCOMP // 2, 16, panels), BF16),
            pltpu.VMEM((4, 32, panels), BF16),
            pltpu.VMEM((BLOCK, panels, 256), BF16),
            pltpu.VMEM((BLOCK, panels, 256), BF16),
            pltpu.SemaphoreType.DMA((6 + STREAMS,)),
        ]
        + [pltpu.VMEM((5, panels // STREAMS, 128), F32)] * STREAMS,
        compiler_params=pltpu.CompilerParams(vmem_limit_bytes=60000000),
        cost_estimate=pl.CostEstimate(flops=20_000_000_000, bytes_accessed=8_000_000, transcendentals=0),
        name="radiate",
    )(zero, table, exchanged, start, blades[None, :])


def regroup_kernel(source_hbm, out_hbm, held, in_sem, out_sem):
    owners, _, width = out_hbm.shape
    parts = 16
    share = owners // parts
    arrive = [
        pltpu.make_async_copy(
            source_hbm.at[:, pl.ds(p * share * width, share * width)],
            held.at[:, pl.ds(p * share * width, share * width)],
            in_sem.at[p],
        )
        for p in range(parts)
    ]
    leave = [
        pltpu.make_async_copy(held.at[:, pl.ds(o * width, width)], out_hbm.at[o], out_sem.at[o])
        for o in range(owners)
    ]
    for c in arrive:
        c.start()
    for p in range(parts):
        arrive[p].wait()
        for o in range(p * share, (p + 1) * share):
            leave[o].start()
    for c in leave:
        c.wait()


def regroup(sources, owners):
    rows, columns = sources.shape
    return pl.pallas_call(
        regroup_kernel,
        out_shape=jax.ShapeDtypeStruct((owners, rows, columns // owners), sources.dtype),
        in_specs=[pl.BlockSpec(memory_space=pltpu.HBM)],
        out_specs=pl.BlockSpec(memory_space=pltpu.HBM),
        scratch_shapes=[
            pltpu.VMEM((rows, columns), sources.dtype),
            pltpu.SemaphoreType.DMA((16,)),
            pltpu.SemaphoreType.DMA((owners,)),
        ],
        compiler_params=pltpu.CompilerParams(vmem_limit_bytes=60_000_000),
        name="regroup",
    )(sources)


def body(sources, panel_pos, panel_blade, observer_table, observer_index):
    owners = lax.axis_size("freq")
    position = lax.axis_index("freq")
    observers = observer_table[:, observer_index]
    width = sources.shape[1] // owners
    blocks = regroup(sources, owners)
    exchanged = lax.all_to_all(blocks, "freq", split_axis=0, concat_axis=0, tiled=True)
    exchanged = exchanged.reshape(-1, width)
    table = transform_table()
    own_pos = lax.dynamic_slice_in_dim(panel_pos, position * width, width, 1)
    own_blade = lax.dynamic_slice_in_dim(panel_blade, position * width, width, 0)
    start = green_start(own_pos, observers)
    partial = radiate(table, exchanged, start, own_blade)
    blocks = partial.reshape(owners * NCOMP, -1, 128).astype(BF16)
    arrived = lax.all_to_all(blocks, ("freq", "grp"), split_axis=0, concat_axis=0, tiled=True)
    total = arrived.astype(F32).sum(0)
    total = total.reshape(-1, 2, QUAD, observers.shape[1]).transpose(0, 2, 1, 3)
    return total.reshape(NF // owners, 1, 2, observers.shape[1])


def solution(mesh):
    in_specs = (P("freq", "grp"), P(None, "grp"), P("grp"), P(), P())
    out_specs = P("freq", "grp", None, None)
    return jax.shard_map(body, mesh=mesh, in_specs=in_specs, out_specs=out_specs, check_vma=False)
```

```python
import functools
import math

import jax
import jax.numpy as jnp
from jax import lax
from jax.experimental import pallas as pl
from jax.experimental.pallas import tpu as pltpu
from jax.sharding import PartitionSpec as P

NT = 1024
NF = 512
NCOMP = 4
QUAD = 4
BLOCK = 16
STREAMS = 2
GROUP = 2
EARLY = 64
POP = 1
F32, BF16 = jnp.float32, jnp.bfloat16

wave_step = 0.04


def transform_table():
    samples = jnp.arange(NT, dtype=jnp.int32)
    low_row = jnp.arange(64, dtype=jnp.int32)
    high_row = jnp.arange(NF // 32, dtype=jnp.int32)
    turn = 2.0 * math.pi / NT
    low_count = ((low_row // 2)[:, None] * samples[None, :] + (NT // 4) * (low_row % 2)[:, None]) % NT
    high_count = 32 * high_row[:, None] * samples[None, :] % NT
    low = turn * low_count.astype(F32)
    high = turn * high_count.astype(F32)
    scale = 1.0 / math.sqrt(NT)
    cl, sl = jnp.cos(low), jnp.sin(low)
    ch, sh = jnp.cos(high) * scale, jnp.sin(high) * scale
    cl, sl, ch, sh = lax.optimization_barrier((cl, sl, ch, sh))
    rows = ch[:, None] * cl[None] - sh[:, None] * sl[None]
    return rows.astype(BF16).reshape(2 * NF, NT)


def prepare_kernel(column_ref, observer_ref, state_ref, green_ref):
    size = column_ref.shape[0]
    offset = (lax.broadcasted_iota(jnp.int32, (size, 128), 1) // 32 - QUAD).astype(F32) * wave_step

    def cos_sin(x):
        x2 = x * x
        c, s = -1.0 / math.factorial(14), -1.0 / math.factorial(15)
        for n in range(6, -1, -1):
            sign = 1.0 if n % 2 == 0 else -1.0
            c = c * x2 + sign / math.factorial(2 * n)
            s = s * x2 + sign / math.factorial(2 * n + 1)
        return c, s * x

    square = None
    for axis in range(3):
        diff = observer_ref[axis : axis + 1, :] - column_ref[:, axis : axis + 1]
        square = diff * diff if square is None else square + diff * diff
    distance = jnp.sqrt(square)
    amplitude = 0.25 / (math.pi * distance)
    cn, sn = cos_sin(offset * distance)
    cq, sq = cos_sin((wave_step * QUAD) * distance)
    c, s = cn * amplitude, -sn * amplitude
    for n, value in enumerate((2.0 * cq, c, s, c * cq - s * sq, s * cq + c * sq)):
        state_ref[n] = value

    def step(i, carry):
        rows = pl.ds(pl.multiple_of(32 * i, 32), 32)
        turn, c, s, cp, sp = [state_ref[n, rows, :] for n in range(5)]
        for k in range(EARLY):
            c, cp = turn * c - cp, c
            s, sp = turn * s - sp, s
            green_ref[k, rows, 0:128] = c.astype(BF16)
            green_ref[k, rows, 128:256] = s.astype(BF16)
        for n, value in enumerate((c, s, cp, sp)):
            state_ref[n + 1, rows, :] = value
        return carry

    lax.fori_loop(0, size // 32, step, 0)


def green_start(positions, observers):
    panels = positions.shape[1]
    size = 128
    return pl.pallas_call(
        prepare_kernel,
        grid=(panels // size,),
        out_shape=(
            jax.ShapeDtypeStruct((5, panels, 128), F32),
            jax.ShapeDtypeStruct((EARLY, panels, 256), BF16),
        ),
        in_specs=[pl.BlockSpec((size, 3), lambda i: (i, 0)), pl.BlockSpec((3, 128), lambda i: (0, 0))],
        out_specs=(
            pl.BlockSpec((5, size, 128), lambda i: (0, i, 0)),
            pl.BlockSpec((EARLY, size, 256), lambda i: (0, i, 0)),
        ),
        compiler_params=pltpu.CompilerParams(vmem_limit_bytes=42_000_000),
        cost_estimate=pl.CostEstimate(flops=5_000_000_000, bytes_accessed=36_000_000, transcendentals=0),
        name="prepare",
    )(positions.T, jnp.tile(observers, (1, QUAD)))


def radiate_kernel(
    zero_ref, table_hbm, source_hbm, start_ref, early_hbm, blade_ref, out_ref,
    table_ref, source_ref, spectrum, masks, weighted, held, green_b, sems, *states
):
    panels = source_ref.shape[1]
    share = panels // STREAMS
    blocks = NF // QUAD // BLOCK
    tiles = panels // 256
    pairs = BLOCK // 2
    chunks = panels // 16
    row = lax.broadcasted_iota(jnp.int32, (8, 128), 0)
    lane = lax.broadcasted_iota(jnp.int32, (8, 128), 1)
    diagonal = (row // 2) == (lane // 32)
    even = (row % 2) == 0
    zero = zero_ref[0]

    table_copies = [
        pltpu.make_async_copy(table_hbm.at[pl.ds(h * NF, NF), :], table_ref.at[pl.ds(h * NF, NF), :], sems.at[h])
        for h in range(2)
    ]
    copies = [
        pltpu.make_async_copy(start_ref.at[:, pl.ds(s * share, share), :], states[s], sems.at[2 + s])
        for s in range(STREAMS)
    ]
    def early_copy(i):
        slot = lax.rem(i, 2)
        return pltpu.make_async_copy(early_hbm.at[pl.ds(i * BLOCK, BLOCK)], held.at[slot], sems.at[6 + STREAMS + slot])

    source_copies = [
        pltpu.make_async_copy(
            source_hbm.at[pl.ds(256 * k, 256), :], source_ref.at[pl.ds(256 * k, 256), :], sems.at[2 + STREAMS + k]
        )
        for k in range(4)
    ]
    for c in [table_copies[0], *source_copies, table_copies[1], early_copy(zero), *copies]:
        c.start()

    def generate(green, stream, slot):
        own = pl.multiple_of(slot * 16, 16)
        rows = pl.ds(own, 16)
        put = pl.ds(pl.multiple_of(own + stream * share, 16), 16)
        state = states[stream]
        turn, c, s, cp, sp = [state[i, rows, :] for i in range(5)]
        for k in range(BLOCK):
            c, cp = turn * c - cp, c
            s, sp = turn * s - sp, s
            green[k, put, 0:128] = c.astype(BF16)
            green[k, put, 128:256] = s.astype(BF16)
        for i, value in enumerate((c, s, cp, sp)):
            state[i + 1, rows, :] = value

    half_row = lax.broadcasted_iota(jnp.int32, (16, panels), 0) // 8
    for p in range(NCOMP // 2):
        masks[p] = jnp.where(blade_ref[...] == half_row + 2 * p, 1.0, 0.0).astype(BF16)

    def transform(*acc):
        half = NF

        def drain(n, h):
            for m in range(2):
                rows = pltpu.matmul_pop(acc[2 * h + m]).reshape(half // 8, 8, 256)
                spectrum[pl.ds(h * half // 8, half // 8), :, pl.ds((2 * n + m) * 256, 256)] = (
                    jnp.concatenate([rows, rows], axis=1).astype(BF16)
                )

        pending = None
        for n in range(tiles // 2):
            for h in range(2):
                if n == 0:
                    table_copies[h].wait()
                for k in range(4):
                    if n == 0 and h == 0:
                        source_copies[k].wait()
                    for m in range(2):
                        pltpu.matmul_push_rhs(
                            source_ref[pl.ds(256 * k, 256), pl.ds((2 * n + m) * 256, 256)],
                            staging_register=k % 2, mxu_index=m,
                        )
                    for m in range(2):
                        pltpu.matmul_acc_lhs(
                            acc[2 * h + m], table_ref[pl.ds(h * half, half), pl.ds(256 * k, 256)],
                            load_staged_rhs=k % 2,
                        )
                    if k == 0 and pending is not None:
                        drain(*pending)
                pending = (n, h)
        drain(*pending)

    pl.run_scoped(
        transform,
        pltpu.ACC(0)((NF, 256), F32), pltpu.ACC(1)((NF, 256), F32),
        pltpu.ACC(0)((NF, 256), F32), pltpu.ACC(1)((NF, 256), F32),
    )

    def weigh(q, slot):
        for m in range(2):
            part = spectrum[jnp.minimum(q + m, NF // QUAD - 1)]
            for p in range(NCOMP // 2):
                weighted[2 * slot + m, pl.ds(16 * p, 16), :] = part * masks[p]

    def merge(a, b, c, d):
        return jnp.where(row < 4, jnp.where(row < 2, a, b), jnp.where(row < 6, c, d))

    def finish(r):
        total = None
        for b in range(NCOMP):
            top = 8 * b
            u = r[top : top + 8, 0:128]
            v = r[top : top + 8, 128:256]
            w = jnp.where(even, -pltpu.roll(v, 7, 0), pltpu.roll(v, 1, 0))
            z = jnp.where(diagonal, u + w, 0.0)
            if b:
                z = pltpu.roll(z, 2 * b, 0)
            total = z if total is None else total + z
        y = total
        for j in range(1, QUAD):
            y = jnp.where(lane // 32 == j, pltpu.roll(total, 8 - 2 * j, 0), y)
        return y

    def contract(*acc):
        trips = pairs // GROUP
        local = chunks // trips // STREAMS

        def trip(block, ii, now, later=None):
            made = 0
            units = [(pair, t) for pair in range(GROUP) for t in range(tiles)]

            def push(pair, t):
                for m in range(2):
                    pltpu.matmul_push_rhs(
                        now[2 * (GROUP * ii + pair) + m, pl.ds(256 * t, 256), :],
                        staging_register=t % 2, mxu_index=m,
                    )

            def accumulate(pair, t):
                for m in range(2):
                    pltpu.matmul_acc_lhs(
                        acc[2 * (pair % 2) + m], weighted[2 * (pair % 2) + m, :, pl.ds(256 * t, 256)],
                        load_staged_rhs=t % 2,
                    )

            def drain(half_q, pair):
                y0, y1 = [finish(pltpu.matmul_pop(acc[2 * (pair % 2) + m])) for m in range(2)]
                upper = merge(y0, pltpu.roll(y1, 2, 0), pltpu.roll(y0, 2, 0), pltpu.roll(y1, 4, 0))
                lower = merge(pltpu.roll(y0, 4, 0), pltpu.roll(y1, 6, 0), pltpu.roll(y0, 6, 0), y1)
                out_ref[half_q] = jnp.concatenate([upper, lower], axis=0).astype(BF16)

            def produce(u):
                if later is None:
                    return
                for n in range(u * local // len(units), (u + 1) * local // len(units)):
                    for stream in range(STREAMS):
                        generate(later, stream, ii * local + lax.rem(zero + n, local))

            for u, (pair, t) in enumerate(units):
                h0 = block * pairs + GROUP * ii + pair
                push(pair, t)
                accumulate(pair, t)
                produce(u)
                if t == POP:
                    weigh(2 * h0 + 2, 1 - pair % 2)
                    if pair:
                        drain(h0 - 1, pair - 1)
            drain(h0, GROUP - 1)

        def step(i, carry):
            @pl.when(i + 1 < blocks // 2)
            def _():
                early_copy(i + 1).start()

            early_copy(i).wait()

            def first(ii, c):
                trip(i, ii, held.at[lax.rem(i, 2)], green_b)
                return c

            lax.fori_loop(0, trips, first, 0)
            weigh((blocks // 2 + i) * BLOCK, 0)

            def second(ii, c):
                trip(blocks // 2 + i, ii, green_b)
                return c

            lax.fori_loop(0, trips, second, 0)
            weigh((i + 1) * BLOCK, 0)
            return carry

        for c in copies:
            c.wait()
        for a in acc:
            pltpu.matmul_pop(a)
        weigh(0, 0)
        lax.fori_loop(0, blocks // 2, step, 0)
    pl.run_scoped(contract, *[pltpu.ACC(n % 2)((32, 256), F32) for n in range(4)])


def radiate(table, exchanged, start, blades):
    start, early = start
    panels = exchanged.shape[1]
    quads = NF // QUAD
    vm = pl.BlockSpec(memory_space=pltpu.VMEM)
    hbm = pl.BlockSpec(memory_space=pltpu.HBM)
    zero = jnp.minimum(blades[:1], 0)
    return pl.pallas_call(
        radiate_kernel,
        out_shape=jax.ShapeDtypeStruct((quads // 2, 4 * NCOMP, 128), BF16),
        in_specs=[pl.BlockSpec(memory_space=pltpu.SMEM), hbm, hbm, hbm, hbm, vm],
        out_specs=vm,
        scratch_shapes=[
            pltpu.VMEM((2 * NF, NT), BF16),
            pltpu.VMEM((NT, panels), BF16),
            pltpu.VMEM((NF // QUAD, 16, panels), BF16),
            pltpu.VMEM((NCOMP // 2, 16, panels), BF16),
            pltpu.VMEM((4, 32, panels), BF16),
            pltpu.VMEM((2, BLOCK, panels, 256), BF16),
            pltpu.VMEM((BLOCK, panels, 256), BF16),
            pltpu.SemaphoreType.DMA((8 + STREAMS,)),
        ]
        + [pltpu.VMEM((5, panels // STREAMS, 128), F32)] * STREAMS,
        compiler_params=pltpu.CompilerParams(vmem_limit_bytes=60000000),
        cost_estimate=pl.CostEstimate(flops=20_000_000_000, bytes_accessed=8_000_000, transcendentals=0),
        name="radiate",
    )(zero, table, exchanged, start, early, blades[None, :])


def regroup_kernel(source_hbm, out_hbm, held, in_sem, out_sem):
    owners, _, width = out_hbm.shape
    parts = 16
    share = owners // parts
    arrive = [
        pltpu.make_async_copy(
            source_hbm.at[:, pl.ds(p * share * width, share * width)],
            held.at[:, pl.ds(p * share * width, share * width)],
            in_sem.at[p],
        )
        for p in range(parts)
    ]
    leave = [
        pltpu.make_async_copy(held.at[:, pl.ds(o * width, width)], out_hbm.at[o], out_sem.at[o])
        for o in range(owners)
    ]
    for c in arrive:
        c.start()
    for p in range(parts):
        arrive[p].wait()
        for o in range(p * share, (p + 1) * share):
            leave[o].start()
    for c in leave:
        c.wait()


def regroup(sources, owners):
    rows, columns = sources.shape
    return pl.pallas_call(
        regroup_kernel,
        out_shape=jax.ShapeDtypeStruct((owners, rows, columns // owners), sources.dtype),
        in_specs=[pl.BlockSpec(memory_space=pltpu.HBM)],
        out_specs=pl.BlockSpec(memory_space=pltpu.HBM),
        scratch_shapes=[
            pltpu.VMEM((rows, columns), sources.dtype),
            pltpu.SemaphoreType.DMA((16,)),
            pltpu.SemaphoreType.DMA((owners,)),
        ],
        compiler_params=pltpu.CompilerParams(vmem_limit_bytes=60_000_000),
        name="regroup",
    )(sources)


def body(sources, panel_pos, panel_blade, observer_table, observer_index):
    owners = lax.axis_size("freq")
    position = lax.axis_index("freq")
    observers = observer_table[:, observer_index]
    width = sources.shape[1] // owners
    blocks = regroup(sources, owners)
    exchanged = lax.all_to_all(blocks, "freq", split_axis=0, concat_axis=0, tiled=True)
    exchanged = exchanged.reshape(-1, width)
    table = transform_table()
    own_pos = lax.dynamic_slice_in_dim(panel_pos, position * width, width, 1)
    own_blade = lax.dynamic_slice_in_dim(panel_blade, position * width, width, 0)
    start = green_start(own_pos, observers)
    partial = radiate(table, exchanged, start, own_blade)
    blocks = partial.reshape(owners * NCOMP, -1, 128)
    arrived = lax.all_to_all(blocks, ("freq", "grp"), split_axis=0, concat_axis=0, tiled=True)
    total = arrived.astype(F32).sum(0)
    total = total.reshape(-1, 2, QUAD, observers.shape[1]).transpose(0, 2, 1, 3)
    return total.reshape(NF // owners, 1, 2, observers.shape[1])


def solution(mesh):
    in_specs = (P("freq", "grp"), P(None, "grp"), P("grp"), P(), P())
    out_specs = P("freq", "grp", None, None)
    return jax.shard_map(body, mesh=mesh, in_specs=in_specs, out_specs=out_specs, check_vma=False)
```

```python
import functools
import math

import jax
import jax.numpy as jnp
from jax import lax
from jax.experimental import pallas as pl
from jax.experimental.pallas import tpu as pltpu
from jax.sharding import PartitionSpec as P

NT = 1024
NF = 512
NCOMP = 4
QUAD = 4
BLOCK = 16
STREAMS = 2
GROUP = 4
EARLY = 64
POP = 1
F32, BF16 = jnp.float32, jnp.bfloat16

wave_step = 0.04


def transform_table():
    samples = jnp.arange(NT, dtype=jnp.int32)
    low_row = jnp.arange(64, dtype=jnp.int32)
    high_row = jnp.arange(NF // 32, dtype=jnp.int32)
    turn = 2.0 * math.pi / NT
    low_count = ((low_row // 2)[:, None] * samples[None, :] + (NT // 4) * (low_row % 2)[:, None]) % NT
    high_count = 32 * high_row[:, None] * samples[None, :] % NT
    low = turn * low_count.astype(F32)
    high = turn * high_count.astype(F32)
    scale = 1.0 / math.sqrt(NT)
    cl, sl = jnp.cos(low), jnp.sin(low)
    ch, sh = jnp.cos(high) * scale, jnp.sin(high) * scale
    cl, sl, ch, sh = lax.optimization_barrier((cl, sl, ch, sh))
    rows = ch[:, None] * cl[None] - sh[:, None] * sl[None]
    return rows.astype(BF16).reshape(2 * NF, NT)


def prepare_kernel(column_ref, observer_ref, state_ref, green_ref):
    size = column_ref.shape[0]
    offset = (lax.broadcasted_iota(jnp.int32, (size, 128), 1) // 32 - QUAD).astype(F32) * wave_step

    def cos_sin(x):
        x2 = x * x
        c, s = -1.0 / math.factorial(14), -1.0 / math.factorial(15)
        for n in range(6, -1, -1):
            sign = 1.0 if n % 2 == 0 else -1.0
            c = c * x2 + sign / math.factorial(2 * n)
            s = s * x2 + sign / math.factorial(2 * n + 1)
        return c, s * x

    square = None
    for axis in range(3):
        diff = observer_ref[axis : axis + 1, :] - column_ref[:, axis : axis + 1]
        square = diff * diff if square is None else square + diff * diff
    distance = jnp.sqrt(square)
    amplitude = 0.25 / (math.pi * distance)
    cn, sn = cos_sin(offset * distance)
    cq, sq = cos_sin((wave_step * QUAD) * distance)
    c, s = cn * amplitude, -sn * amplitude
    for n, value in enumerate((2.0 * cq, c, s, c * cq - s * sq, s * cq + c * sq)):
        state_ref[n] = value

    def step(i, carry):
        rows = pl.ds(pl.multiple_of(32 * i, 32), 32)
        turn, c, s, cp, sp = [state_ref[n, rows, :] for n in range(5)]
        for k in range(EARLY):
            c, cp = turn * c - cp, c
            s, sp = turn * s - sp, s
            green_ref[k, rows, 0:128] = c.astype(BF16)
            green_ref[k, rows, 128:256] = s.astype(BF16)
        for n, value in enumerate((c, s, cp, sp)):
            state_ref[n + 1, rows, :] = value
        return carry

    lax.fori_loop(0, size // 32, step, 0)


def green_start(positions, observers):
    panels = positions.shape[1]
    size = 128
    return pl.pallas_call(
        prepare_kernel,
        grid=(panels // size,),
        out_shape=(
            jax.ShapeDtypeStruct((5, panels, 128), F32),
            jax.ShapeDtypeStruct((EARLY, panels, 256), BF16),
        ),
        in_specs=[pl.BlockSpec((size, 3), lambda i: (i, 0)), pl.BlockSpec((3, 128), lambda i: (0, 0))],
        out_specs=(
            pl.BlockSpec((5, size, 128), lambda i: (0, i, 0)),
            pl.BlockSpec((EARLY, size, 256), lambda i: (0, i, 0)),
        ),
        compiler_params=pltpu.CompilerParams(vmem_limit_bytes=42_000_000),
        cost_estimate=pl.CostEstimate(flops=5_000_000_000, bytes_accessed=36_000_000, transcendentals=0),
        name="prepare",
    )(positions.T, jnp.tile(observers, (1, QUAD)))


def radiate_kernel(
    zero_ref, table_hbm, source_hbm, start_ref, early_hbm, blade_ref, out_ref,
    table_ref, source_ref, spectrum, masks, weighted, held, green_b, sems, *states
):
    panels = source_ref.shape[1]
    share = panels // STREAMS
    blocks = NF // QUAD // BLOCK
    tiles = panels // 256
    pairs = BLOCK // 2
    chunks = panels // 16
    row = lax.broadcasted_iota(jnp.int32, (8, 128), 0)
    lane = lax.broadcasted_iota(jnp.int32, (8, 128), 1)
    diagonal = (row // 2) == (lane // 32)
    even = (row % 2) == 0
    zero = zero_ref[0]

    table_copies = [
        pltpu.make_async_copy(table_hbm.at[pl.ds(h * NF, NF), :], table_ref.at[pl.ds(h * NF, NF), :], sems.at[h])
        for h in range(2)
    ]
    copies = [
        pltpu.make_async_copy(start_ref.at[:, pl.ds(s * share, share), :], states[s], sems.at[2 + s])
        for s in range(STREAMS)
    ]
    def early_copy(i):
        slot = lax.rem(i, 2)
        return pltpu.make_async_copy(early_hbm.at[pl.ds(i * BLOCK, BLOCK)], held.at[slot], sems.at[6 + STREAMS + slot])

    source_copies = [
        pltpu.make_async_copy(
            source_hbm.at[pl.ds(256 * k, 256), :], source_ref.at[pl.ds(256 * k, 256), :], sems.at[2 + STREAMS + k]
        )
        for k in range(4)
    ]
    for c in [table_copies[0], *source_copies, table_copies[1], early_copy(zero), *copies]:
        c.start()

    def generate(green, stream, slot):
        own = pl.multiple_of(slot * 16, 16)
        rows = pl.ds(own, 16)
        put = pl.ds(pl.multiple_of(own + stream * share, 16), 16)
        state = states[stream]
        turn, c, s, cp, sp = [state[i, rows, :] for i in range(5)]
        for k in range(BLOCK):
            c, cp = turn * c - cp, c
            s, sp = turn * s - sp, s
            green[k, put, 0:128] = c.astype(BF16)
            green[k, put, 128:256] = s.astype(BF16)
        for i, value in enumerate((c, s, cp, sp)):
            state[i + 1, rows, :] = value

    half_row = lax.broadcasted_iota(jnp.int32, (16, panels), 0) // 8
    for p in range(NCOMP // 2):
        masks[p] = jnp.where(blade_ref[...] == half_row + 2 * p, 1.0, 0.0).astype(BF16)

    def transform(*acc):
        half = NF

        def drain(n, h):
            for m in range(2):
                rows = pltpu.matmul_pop(acc[2 * h + m]).reshape(half // 8, 8, 256)
                spectrum[pl.ds(h * half // 8, half // 8), :, pl.ds((2 * n + m) * 256, 256)] = (
                    jnp.concatenate([rows, rows], axis=1).astype(BF16)
                )

        pending = None
        for n in range(tiles // 2):
            for h in range(2):
                if n == 0:
                    table_copies[h].wait()
                for k in range(4):
                    if n == 0 and h == 0:
                        source_copies[k].wait()
                    for m in range(2):
                        pltpu.matmul_push_rhs(
                            source_ref[pl.ds(256 * k, 256), pl.ds((2 * n + m) * 256, 256)],
                            staging_register=k % 2, mxu_index=m,
                        )
                    for m in range(2):
                        pltpu.matmul_acc_lhs(
                            acc[2 * h + m], table_ref[pl.ds(h * half, half), pl.ds(256 * k, 256)],
                            load_staged_rhs=k % 2,
                        )
                    if k == 0 and pending is not None:
                        drain(*pending)
                pending = (n, h)
        drain(*pending)

    pl.run_scoped(
        transform,
        pltpu.ACC(0)((NF, 256), F32), pltpu.ACC(1)((NF, 256), F32),
        pltpu.ACC(0)((NF, 256), F32), pltpu.ACC(1)((NF, 256), F32),
    )

    def weigh(q, slot):
        for m in range(2):
            part = spectrum[jnp.minimum(q + m, NF // QUAD - 1)]
            for p in range(NCOMP // 2):
                weighted[2 * slot + m, pl.ds(16 * p, 16), :] = part * masks[p]

    def merge(a, b, c, d):
        return jnp.where(row < 4, jnp.where(row < 2, a, b), jnp.where(row < 6, c, d))

    def finish(r):
        total = None
        for b in range(NCOMP):
            top = 8 * b
            u = r[top : top + 8, 0:128]
            v = r[top : top + 8, 128:256]
            w = jnp.where(even, -pltpu.roll(v, 7, 0), pltpu.roll(v, 1, 0))
            z = jnp.where(diagonal, u + w, 0.0)
            if b:
                z = pltpu.roll(z, 2 * b, 0)
            total = z if total is None else total + z
        y = total
        for j in range(1, QUAD):
            y = jnp.where(lane // 32 == j, pltpu.roll(total, 8 - 2 * j, 0), y)
        return y

    def contract(*acc):
        trips = pairs // GROUP
        local = chunks // trips // STREAMS

        def trip(block, ii, group, now, later=None):
            made = 0
            units = [(pair, t) for pair in range(group) for t in range(tiles)]

            def push(pair, t):
                for m in range(2):
                    pltpu.matmul_push_rhs(
                        now[2 * (group * ii + pair) + m, pl.ds(256 * t, 256), :],
                        staging_register=t % 2, mxu_index=m,
                    )

            def accumulate(pair, t):
                for m in range(2):
                    pltpu.matmul_acc_lhs(
                        acc[2 * (pair % 2) + m], weighted[2 * (pair % 2) + m, :, pl.ds(256 * t, 256)],
                        load_staged_rhs=t % 2,
                    )

            def drain(half_q, pair):
                y0, y1 = [finish(pltpu.matmul_pop(acc[2 * (pair % 2) + m])) for m in range(2)]
                upper = merge(y0, pltpu.roll(y1, 2, 0), pltpu.roll(y0, 2, 0), pltpu.roll(y1, 4, 0))
                lower = merge(pltpu.roll(y0, 4, 0), pltpu.roll(y1, 6, 0), pltpu.roll(y0, 6, 0), y1)
                out_ref[half_q] = jnp.concatenate([upper, lower], axis=0).astype(BF16)

            def produce(u):
                if later is None:
                    return
                for n in range(u * local // len(units), (u + 1) * local // len(units)):
                    for stream in range(STREAMS):
                        generate(later, stream, ii * local + lax.rem(zero + n, local))

            for u, (pair, t) in enumerate(units):
                h0 = block * pairs + group * ii + pair
                push(pair, t)
                accumulate(pair, t)
                produce(u)
                if t == POP:
                    weigh(2 * h0 + 2, 1 - pair % 2)
                    if pair:
                        drain(h0 - 1, pair - 1)
            drain(h0, group - 1)

        def step(i, carry):
            @pl.when(i + 1 < blocks // 2)
            def _():
                early_copy(i + 1).start()

            early_copy(i).wait()

            def first(ii, c):
                trip(i, ii, GROUP, held.at[lax.rem(i, 2)], green_b)
                return c

            lax.fori_loop(0, trips, first, 0)
            weigh((blocks // 2 + i) * BLOCK, 0)

            trip(blocks // 2 + i, 0, pairs, green_b)
            weigh((i + 1) * BLOCK, 0)
            return carry

        for c in copies:
            c.wait()
        for a in acc:
            pltpu.matmul_pop(a)
        weigh(0, 0)
        lax.fori_loop(0, blocks // 2, step, 0)
    pl.run_scoped(contract, *[pltpu.ACC(n % 2)((32, 256), F32) for n in range(4)])


def radiate(table, exchanged, start, blades):
    start, early = start
    panels = exchanged.shape[1]
    quads = NF // QUAD
    vm = pl.BlockSpec(memory_space=pltpu.VMEM)
    hbm = pl.BlockSpec(memory_space=pltpu.HBM)
    zero = jnp.minimum(blades[:1], 0)
    return pl.pallas_call(
        radiate_kernel,
        out_shape=jax.ShapeDtypeStruct((quads // 2, 4 * NCOMP, 128), BF16),
        in_specs=[pl.BlockSpec(memory_space=pltpu.SMEM), hbm, hbm, hbm, hbm, vm],
        out_specs=vm,
        scratch_shapes=[
            pltpu.VMEM((2 * NF, NT), BF16),
            pltpu.VMEM((NT, panels), BF16),
            pltpu.VMEM((NF // QUAD, 16, panels), BF16),
            pltpu.VMEM((NCOMP // 2, 16, panels), BF16),
            pltpu.VMEM((4, 32, panels), BF16),
            pltpu.VMEM((2, BLOCK, panels, 256), BF16),
            pltpu.VMEM((BLOCK, panels, 256), BF16),
            pltpu.SemaphoreType.DMA((8 + STREAMS,)),
        ]
        + [pltpu.VMEM((5, panels // STREAMS, 128), F32)] * STREAMS,
        compiler_params=pltpu.CompilerParams(vmem_limit_bytes=60000000),
        cost_estimate=pl.CostEstimate(flops=20_000_000_000, bytes_accessed=8_000_000, transcendentals=0),
        name="radiate",
    )(zero, table, exchanged, start, early, blades[None, :])


def regroup_kernel(source_hbm, out_hbm, held, in_sem, out_sem):
    owners, _, width = out_hbm.shape
    parts = 16
    share = owners // parts
    arrive = [
        pltpu.make_async_copy(
            source_hbm.at[:, pl.ds(p * share * width, share * width)],
            held.at[:, pl.ds(p * share * width, share * width)],
            in_sem.at[p],
        )
        for p in range(parts)
    ]
    leave = [
        pltpu.make_async_copy(held.at[:, pl.ds(o * width, width)], out_hbm.at[o], out_sem.at[o])
        for o in range(owners)
    ]
    for c in arrive:
        c.start()
    for p in range(parts):
        arrive[p].wait()
        for o in range(p * share, (p + 1) * share):
            leave[o].start()
    for c in leave:
        c.wait()


def regroup(sources, owners):
    rows, columns = sources.shape
    return pl.pallas_call(
        regroup_kernel,
        out_shape=jax.ShapeDtypeStruct((owners, rows, columns // owners), sources.dtype),
        in_specs=[pl.BlockSpec(memory_space=pltpu.HBM)],
        out_specs=pl.BlockSpec(memory_space=pltpu.HBM),
        scratch_shapes=[
            pltpu.VMEM((rows, columns), sources.dtype),
            pltpu.SemaphoreType.DMA((16,)),
            pltpu.SemaphoreType.DMA((owners,)),
        ],
        compiler_params=pltpu.CompilerParams(vmem_limit_bytes=60_000_000),
        name="regroup",
    )(sources)


def body(sources, panel_pos, panel_blade, observer_table, observer_index):
    owners = lax.axis_size("freq")
    position = lax.axis_index("freq")
    observers = observer_table[:, observer_index]
    width = sources.shape[1] // owners
    blocks = regroup(sources, owners)
    exchanged = lax.all_to_all(blocks, "freq", split_axis=0, concat_axis=0, tiled=True)
    exchanged = exchanged.reshape(-1, width)
    table = transform_table()
    own_pos = lax.dynamic_slice_in_dim(panel_pos, position * width, width, 1)
    own_blade = lax.dynamic_slice_in_dim(panel_blade, position * width, width, 0)
    start = green_start(own_pos, observers)
    partial = radiate(table, exchanged, start, own_blade)
    blocks = partial.reshape(owners * NCOMP, -1, 128)
    arrived = lax.all_to_all(blocks, ("freq", "grp"), split_axis=0, concat_axis=0, tiled=True)
    total = arrived.astype(F32).sum(0)
    total = total.reshape(-1, 2, QUAD, observers.shape[1]).transpose(0, 2, 1, 3)
    return total.reshape(NF // owners, 1, 2, observers.shape[1])


def solution(mesh):
    in_specs = (P("freq", "grp"), P(None, "grp"), P("grp"), P(), P())
    out_specs = P("freq", "grp", None, None)
    return jax.shard_map(body, mesh=mesh, in_specs=in_specs, out_specs=out_specs, check_vma=False)
```
